32 devices in a mesh: dp: 8 (over z, y), mp: 4 (over x, core).
Axes of the slice: x: 2, y: 2, z: 4, core: 2. Of those that a mesh axis runs over, the one named last changes fastest.
Arguments:
- queries: bfloat16 [24576, 2048], P('dp', 'mp'), may hold values from -30 to 30
- keys: bfloat16 [24576, 512], P('dp', 'mp'), may hold values from -30 to 30
- values: bfloat16 [24576, 512], P('dp', 'mp'), may hold values from -6 to 6
- doc_ids: int32 [24576], P('dp'), may hold values from -1 to 127, as said below
- live_counts: int32 [8], P('dp'), may hold values from 1 to 24, 176 in all
- out_weight: bfloat16 [2048, 4096], P('dp', 'mp'), may hold values from -0.125 to 0.125
Outputs:
- mixed: bfloat16 [22528, 4096], P('dp', 'mp')
The draws below stay inside these ranges and needn't reach their ends.
Inputs may be any that keep to these rules, and one draw needn't show every extreme that they name: `live_counts`: each device has 1 to 24 live blocks, 176 in all, and some device has exactly 24. `doc_ids`: within each block the numbers start at 0 and never fall along the block, and the -1 entries, if any, form the block's tail.
All inputs are finite; a program needn't handle non-finite values.
Results may differ from the reference program's by a relative error of at most 0.0049.
Values may be sent and summed in bfloat16 or wider, within the bound.
A program may use at most 128 MiB of HBM per device.

```python
import math
import jax
import jax.numpy as jnp
import numpy as np
from jax import lax

D = 4096
HEAD_SIZE = 128
HQ = 16
KEY_VALUE_HEADS = 4
BLOCK = 128
NB = 24
RCAP = 22
TOKEN_POSITIONS = 24576
N_DP = 8


def draw_queries(key, part):
    drawn_result = jnp.clip(jax.random.normal(jax.random.fold_in(key, 1), (TOKEN_POSITIONS, HQ * HEAD_SIZE), jnp.float32), -6.0, 6.0)
    return drawn_result.astype(jnp.bfloat16)


def draw_keys(key, part):
    drawn_result = jnp.clip(jax.random.normal(jax.random.fold_in(key, 2), (TOKEN_POSITIONS, KEY_VALUE_HEADS * HEAD_SIZE), jnp.float32), -6.0, 6.0)
    return drawn_result.astype(jnp.bfloat16)


def draw_doc_ids(key, part):
    blocks = TOKEN_POSITIONS // BLOCK
    places = jnp.arange(BLOCK, dtype=jnp.int32)[None, :]
    cuts = jax.random.randint(jax.random.fold_in(key, 21), (blocks, BLOCK), 0, 24) == 0
    cuts = cuts & (places > 0)
    numbers = jnp.cumsum(cuts.astype(jnp.int32), axis=1).astype(jnp.int32)
    filled = jax.random.randint(jax.random.fold_in(key, 22), (blocks, 1), BLOCK // 2, BLOCK + 1)
    numbers = jnp.where(places < filled, numbers, -1)
    first_block = jnp.arange(blocks, dtype=jnp.int32)[:, None] == 0
    numbers = jnp.where(first_block, places, numbers)
    return numbers.reshape(TOKEN_POSITIONS).astype(jnp.int32)


def levels(own_key, dims, shards, least, largest):
    factor_of, own = 1.0, jax.random.fold_in(own_key, 6)
    for axis_at, shards_of in shards:
        heights = jnp.exp(jax.random.uniform(jax.random.fold_in(own, axis_at), (shards_of,), jnp.float32, least / len(shards), largest / len(shards)))
        factor_of = factor_of * jnp.repeat(heights, dims[axis_at] // shards_of).reshape([-1 if axis == axis_at else 1 for axis in range(len(dims))])
    return factor_of


def profile(count, total, most, skew):
    loads = [(1 << 20) // math.isqrt(standing ** skew) + 1 for standing in range(2, count + 1)]
    rest, counts = total - most - (count - 1), [1] * (count - 1)
    while rest > 0:
        free = [i for i in range(count - 1) if counts[i] < most]
        whole, remaining = sum([loads[i] for i in free]), rest
        for i in free:
            more = min(most - counts[i], max(1, remaining * loads[i] // whole), rest)
            counts[i] = counts[i] + more
            rest = rest - more
    return np.array([most] + counts)


def uneven(rng, amount, total, bound, skew):
    if amount == 2:
        one = jax.random.randint(rng, (), max(1, total - bound), min(bound, total - 1) + 1)
        return jnp.stack([one, total - one])
    lengths = jnp.asarray(profile(amount, total, bound, skew), jnp.int32)
    pairs = (amount - 1) // 2
    donor, sink = lengths[1:1 + 2 * pairs:2], lengths[2:2 + 2 * pairs:2]
    room = jnp.minimum(donor - 1, bound - sink)
    shifted = jax.random.randint(jax.random.fold_in(rng, 1), (pairs,), 0, 1 << 20) % (room + 1)
    lengths = lengths.at[1:1 + 2 * pairs:2].set(donor - shifted).at[2:2 + 2 * pairs:2].set(sink + shifted)
    return lengths[jax.random.permutation(jax.random.fold_in(rng, 2), amount)]


def gaussian(key, dims, spread, limit, shards=(), held_as=jnp.bfloat16):
    level = levels(key, dims, shards, -0.22, 0.18) if shards else 1.0
    values = jax.random.normal(key, dims, jnp.float32) * spread * level
    return jnp.minimum(jnp.maximum(values, -limit), limit).astype(held_as)


def setup_inputs(seed: int = 0) -> dict:
    key_of = jax.random.split(jax.random.key(seed), 7)
    return {
        "queries": draw_queries(jax.random.fold_in(key_of[6], 71), 0),
        "keys": draw_keys(jax.random.fold_in(key_of[6], 71), 0),
        "values": gaussian(key_of[2], (TOKEN_POSITIONS, KEY_VALUE_HEADS * HEAD_SIZE), 1.0, 6.0, ((0, 8), (1, 4))),
        "doc_ids": draw_doc_ids(jax.random.fold_in(key_of[6], 71), 0),
        "live_counts": uneven(key_of[4], N_DP, N_DP * RCAP, NB, 2).astype(jnp.int32),
        "out_weight": gaussian(key_of[5], (HQ * HEAD_SIZE, D), (HQ * HEAD_SIZE) ** -0.5, 0.125, ((0, 8), (1, 4))),
    }


masked_score = -1e+30

def attend_blocks(query_blocks, key_blocks, value_blocks, id_blocks):
    number = query_blocks.shape[0]
    query_heads = query_blocks.shape[2] // HEAD_SIZE
    key_heads = key_blocks.shape[2] // HEAD_SIZE
    repeat = query_heads // key_heads
    query_four = query_blocks.astype(jnp.float32).reshape(number, BLOCK, key_heads, repeat, HEAD_SIZE)
    key_four = key_blocks.astype(jnp.float32).reshape(number, BLOCK, key_heads, HEAD_SIZE)
    value_four = value_blocks.astype(jnp.float32).reshape(number, BLOCK, key_heads, HEAD_SIZE)
    scores = jnp.einsum('bihrd,bjhd->bhrij', query_four, key_four) / math.sqrt(HEAD_SIZE)
    places = jnp.arange(BLOCK, dtype=jnp.int32)
    causal = places[None, :] <= places[:, None]
    allowed = (id_blocks[:, :, None] == id_blocks[:, None, :]) & causal[None]
    scores = jnp.where(allowed[:, None, None], scores, masked_score)
    highest = lax.optimization_barrier(jnp.max(scores, axis=-1, keepdims=True))
    weights = jnp.where(allowed[:, None, None], jnp.exp(scores - highest), 0.0)
    total_counts = lax.optimization_barrier(jnp.sum(weights, axis=-1))
    rounded_counts = lax.optimization_barrier(weights.astype(jnp.bfloat16)).astype(jnp.float32)
    summed = jnp.einsum('bhrij,bjhd->bihrd', rounded_counts, value_four)
    summed = summed / jnp.transpose(total_counts, (0, 3, 1, 2))[..., None]
    summed = jnp.where(id_blocks[:, :, None, None, None] >= 0, summed, 0.0)
    return summed.reshape(number, BLOCK, query_heads * HEAD_SIZE).astype(jnp.bfloat16)

def reference(queries, keys, values, doc_ids, live_counts, out_weight):
    inclusive = jnp.cumsum(live_counts).astype(jnp.int32)
    exclusive = inclusive - live_counts
    owners = jnp.arange(N_DP, dtype=jnp.int32)[:, None]
    places = jnp.arange(RCAP, dtype=jnp.int32)[None, :]
    labels = (places * N_DP + owners).reshape(-1)
    holder = lax.optimization_barrier(jnp.sum((inclusive[None, :] <= labels[:, None]).astype(jnp.int32), axis=1))
    within = labels - exclusive[holder]
    chosen = (holder * NB + within).astype(jnp.int32)
    query_blocks = queries.reshape(N_DP * NB, BLOCK, -1)[chosen]
    key_blocks = keys.reshape(N_DP * NB, BLOCK, -1)[chosen]
    value_blocks = values.reshape(N_DP * NB, BLOCK, -1)[chosen]
    id_blocks = doc_ids.reshape(N_DP * NB, BLOCK)[chosen]

    def owner_rows(operands):
        attended = attend_blocks(operands[0], operands[1], operands[2], operands[3])
        flattened = attended.reshape(RCAP * BLOCK, HQ * HEAD_SIZE)
        return jnp.dot(flattened, out_weight, preferred_element_type=jnp.float32).astype(jnp.bfloat16)
    stacked = lax.map(owner_rows, (query_blocks.reshape(N_DP, RCAP, BLOCK, -1), key_blocks.reshape(N_DP, RCAP, BLOCK, -1), value_blocks.reshape(N_DP, RCAP, BLOCK, -1), id_blocks.reshape(N_DP, RCAP, BLOCK)))
    return stacked.reshape(N_DP * RCAP * BLOCK, D)
```

```python
import functools
import math

import jax
import jax.numpy as jnp
from jax import lax
from jax.experimental import pallas as pl
from jax.experimental.pallas import tpu as pltpu
from jax.sharding import PartitionSpec as P

HEAD_SIZE = 128
BLOCK = 128
NB = 24
MESH = pl.DeviceIdType.MESH
MASKED = -1e30


def attend_kernel(per_owner, chosen_ref, queries_ref, keys_ref, values_ref, ids_ref, out_ref):
    step = pl.program_id(0)
    repeat = queries_ref.shape[1] // HEAD_SIZE
    factor = math.log2(math.e) / math.sqrt(HEAD_SIZE)
    row_at = lax.broadcasted_iota(jnp.int32, (BLOCK, BLOCK), 0)
    col_at = lax.broadcasted_iota(jnp.int32, (BLOCK, BLOCK), 1)
    causal = col_at <= row_at
    for layer in range(per_owner):
        block = chosen_ref[step * per_owner + layer]
        rows = pl.ds(pl.multiple_of(block * BLOCK, BLOCK), BLOCK)
        along = jnp.broadcast_to(ids_ref[pl.ds(block, 1), :], (BLOCK, BLOCK))
        down = along.T
        allowed = (along == down) & causal
        real = down >= 0
        key = keys_ref[rows, :]
        value = values_ref[rows, :]
        for head in range(repeat):
            columns = slice(head * HEAD_SIZE, (head + 1) * HEAD_SIZE)
            query = queries_ref[rows, columns]
            scores = lax.dot_general(
                query, key, (((1,), (1,)), ((), ())), preferred_element_type=jnp.float32
            )
            scores = jnp.where(allowed, scores, MASKED)
            highest = jnp.max(scores, axis=1, keepdims=True)
            weights = jnp.exp2((scores - highest) * factor)
            totals = jnp.sum(weights, axis=1, keepdims=True)
            summed = jnp.dot(
                weights.astype(jnp.bfloat16), value, preferred_element_type=jnp.float32
            )
            summed = jnp.where(real, summed / totals, 0.0)
            out_ref[0, layer, :, columns] = summed.astype(out_ref.dtype)


def attend(chosen, queries, keys, values, ids, members, per_owner):
    cols = queries.shape[1]

    def whole(array):
        return pl.BlockSpec(array.shape, lambda i, c: (0, 0))

    return pl.pallas_call(
        functools.partial(attend_kernel, per_owner),
        out_shape=jax.ShapeDtypeStruct((members, per_owner, BLOCK, cols), jnp.bfloat16),
        grid_spec=pltpu.PrefetchScalarGridSpec(
            num_scalar_prefetch=1,
            grid=(members,),
            in_specs=[whole(queries), whole(keys), whole(values), whole(ids)],
            out_specs=pl.BlockSpec((1, per_owner, BLOCK, cols), lambda i, c: (i, 0, 0, 0)),
        ),
        compiler_params=pltpu.CompilerParams(vmem_limit_bytes=40 * 1024 * 1024),
        cost_estimate=pl.CostEstimate(
            flops=members * per_owner * cols * BLOCK * BLOCK * 4,
            bytes_accessed=4 * queries.size,
            transcendentals=members * per_owner * cols * BLOCK,
        ),
    )(chosen, queries, keys, values, ids)


def flip(index, mask):
    bit = 1
    while bit <= mask:
        if mask & bit:
            index = index + bit - 2 * bit * ((index // bit) % 2)
        bit *= 2
    return index


def exchange_kernel(
    members, columns, per_owner,
    sent_ref, weight_ref, far_weight_ref, held_ref, full_ref,
    local_sem, send_dp, recv_dp, send_x, recv_x, send_w, recv_w,
):
    me = lax.axis_index("dp")
    mine = lax.axis_index("mp")
    top = members // 2

    def dp_device(mask):
        return (flip(me, mask), mine)

    def mp_device(mask):
        return (me, flip(mine, mask))

    bits = [1 << b for b in reversed(range(columns.bit_length() - 1))]
    barrier = pltpu.get_barrier_semaphore()
    for mask in range(1, members):
        pl.semaphore_signal(barrier, inc=1, device_id=dp_device(mask), device_id_type=MESH)
    for mask in bits:
        pl.semaphore_signal(barrier, inc=1, device_id=mp_device(mask), device_id_type=MESH)
    pl.semaphore_wait(barrier, members - 1 + len(bits))

    def dp_copy(mask, layer, source):
        return pltpu.make_async_remote_copy(
            src_ref=sent_ref.at[flip(me, mask), layer],
            dst_ref=held_ref.at[mine, source, layer],
            send_sem=send_dp.at[mask, layer],
            recv_sem=recv_dp.at[mask, layer],
            device_id=dp_device(mask),
            device_id_type=MESH,
        )

    def mp_copy(place, bit, mask, layer):
        source = flip(me, mask)
        column = flip(mine, place)
        if mask == 0 and place == 0:
            src = sent_ref.at[source, layer]
        else:
            src = held_ref.at[column, source, layer]
        return pltpu.make_async_remote_copy(
            src_ref=src,
            dst_ref=held_ref.at[column, source, layer],
            send_sem=send_x.at[place ^ bit, mask, layer],
            recv_sem=recv_x.at[place ^ bit, mask, layer],
            device_id=mp_device(bit),
            device_id_type=MESH,
        )

    def weight_copy(mask, bit):
        owner = flip(me, mask)
        if mask == 0:
            src = weight_ref
        elif mask == top:
            src = far_weight_ref
        else:
            src = full_ref.at[owner]
        return pltpu.make_async_remote_copy(
            src_ref=src,
            dst_ref=full_ref.at[owner],
            send_sem=send_w.at[mask ^ bit],
            recv_sem=recv_w.at[mask ^ bit],
            device_id=dp_device(bit),
            device_id_type=MESH,
        )

    local = [
        pltpu.make_async_copy(weight_ref, full_ref.at[me], local_sem.at[0]),
        pltpu.make_async_copy(far_weight_ref, full_ref.at[flip(me, top)], local_sem.at[1]),
        pltpu.make_async_copy(sent_ref.at[me], held_ref.at[mine, me], local_sem.at[2]),
    ]
    started = []

    def start(copy):
        copy.start()
        started.append(copy)

    def spread_weight(mask, below):
        bit = below // 2
        while bit >= 1:
            start(weight_copy(mask, bit))
            bit //= 2

    def spread(place, below, mask, layer):
        for bit in bits:
            if bit < below:
                start(mp_copy(place, bit, mask, layer))

    order = sorted(range(1, members), key=lambda t: (-(bin(t).count("1") % 2), t))
    spread_weight(0, top)
    spread_weight(top, top)
    for layer in range(per_owner):
        spread(0, columns, 0, layer)
        for mask in order:
            start(dp_copy(mask, layer, me))
    for copy in local:
        copy.start()

    chunks = [(0, layer) for layer in range(per_owner)]
    chunks += [(mask, layer) for layer in range(per_owner) for mask in order]
    weights = [t for t in range(1, members) if t != top]
    weights.sort(key=lambda t: (-(t & -t), t))
    lag = 3

    def relay(mask, layer):
        for place in range(1, columns):
            lowest = place & -place
            mp_copy(place ^ lowest, lowest, mask, layer).wait_recv()
            spread(place, lowest, mask, layer)

    for at in range(len(chunks) + lag):
        if at < len(chunks):
            mask, layer = chunks[at]
            if mask:
                dp_copy(mask, layer, me).wait_recv()
                spread(0, columns, mask, layer)
        if at % 3 == 2 and weights:
            arrived = weights.pop(0)
            lowest = arrived & -arrived
            weight_copy(arrived ^ lowest, lowest).wait_recv()
            spread_weight(arrived, lowest)
        if at >= lag:
            relay(*chunks[at - lag])
    for arrived in weights:
        lowest = arrived & -arrived
        weight_copy(arrived ^ lowest, lowest).wait_recv()
        spread_weight(arrived, lowest)
    for copy in started:
        copy.wait_send()
    for copy in local:
        copy.wait()


def exchange(sent, weight, far_weight, members, columns):
    per_owner = sent.shape[1]
    anywhere = pl.BlockSpec(memory_space=pl.ANY)
    dma = pltpu.SemaphoreType.DMA
    return pl.pallas_call(
        functools.partial(exchange_kernel, members, columns, per_owner),
        out_shape=(
            jax.ShapeDtypeStruct((columns,) + sent.shape, sent.dtype),
            jax.ShapeDtypeStruct((members,) + weight.shape, weight.dtype),
        ),
        in_specs=[anywhere] * 3,
        out_specs=(anywhere, anywhere),
        scratch_shapes=[
            dma((3,)),
            dma((members, per_owner)),
            dma((members, per_owner)),
            dma((columns, members, per_owner)),
            dma((columns, members, per_owner)),
            dma((members,)),
            dma((members,)),
        ],
        compiler_params=pltpu.CompilerParams(collective_id=0, has_side_effects=True),
        cost_estimate=pl.CostEstimate(
            flops=0, bytes_accessed=60 * sent.size, transcendentals=0
        ),
    )(sent, weight, far_weight)


def project_kernel(columns, slots_ref, first_ref, second_ref, weight_ref, out_ref):
    total = None
    for column in range(columns):
        rows = jnp.concatenate([first_ref[column, 0], second_ref[column, 0]], axis=0)
        depth = rows.shape[1]
        part = jnp.dot(
            rows, weight_ref[column * depth:(column + 1) * depth, :],
            preferred_element_type=jnp.float32,
        )
        total = part if total is None else total + part
    out_ref[...] = total.astype(out_ref.dtype)


def project(slots, held, weight, kept):
    columns, total, _, depth = held.shape
    width = weight.shape[1]

    def picked(which):
        return pl.BlockSpec(
            (columns, 1, BLOCK, depth), lambda i, s: (0, s[2 * i + which], 0, 0)
        )

    return pl.pallas_call(
        functools.partial(project_kernel, columns),
        out_shape=jax.ShapeDtypeStruct((kept * BLOCK, width), jnp.bfloat16),
        grid_spec=pltpu.PrefetchScalarGridSpec(
            num_scalar_prefetch=1,
            grid=(kept // 2,),
            in_specs=[
                picked(0),
                picked(1),
                pl.BlockSpec(weight.shape, lambda i, s: (0, 0)),
            ],
            out_specs=pl.BlockSpec((2 * BLOCK, width), lambda i, s: (i, 0)),
        ),
        compiler_params=pltpu.CompilerParams(vmem_limit_bytes=40 * 1024 * 1024),
    )(slots, held, held, weight)


def body(members, columns, queries, keys, values, doc_ids, live_counts, out_weight):
    per_owner = (NB + members - 1) // members
    kept = NB * 11 // 12
    own = lax.axis_index("dp")
    half = members // 2
    far_weight = lax.ppermute(
        out_weight, "dp", [(i, (i + half) % members) for i in range(members)]
    )
    table = lax.all_gather(live_counts, "dp", axis=0, tiled=True)
    places = jnp.arange(members, dtype=jnp.int32)
    before = places[None, :] < places[:, None]
    starts = jnp.sum(jnp.where(before, table[None, :], 0), axis=1)
    first_label = jnp.sum(jnp.where(places < own, table, 0))
    owners = jnp.arange(members, dtype=jnp.int32)[:, None]
    layers = jnp.arange(per_owner, dtype=jnp.int32)[None, :]
    chosen = ((owners - first_label) % members + layers * members).reshape(-1)
    chosen = jnp.minimum(chosen, NB - 1)
    wanted = own + jnp.arange(kept, dtype=jnp.int32) * members
    within = wanted[:, None] - starts[None, :]
    holds = (within >= 0) & (within < table[None, :])
    slots = jnp.sum(
        jnp.where(holds, places[None, :] * per_owner + within // members, 0), axis=1
    )
    sent = attend(
        chosen, queries, keys, values, doc_ids.reshape(NB, BLOCK), members, per_owner
    )
    held, full = exchange(sent, out_weight, far_weight, members, columns)
    held = held.reshape(columns, members * per_owner, BLOCK, queries.shape[1])
    full = full.reshape(members * out_weight.shape[0], out_weight.shape[1])
    return project(slots, held, full, kept)


def solution(mesh):
    return jax.shard_map(
        functools.partial(body, mesh.shape["dp"], mesh.shape["mp"]),
        mesh=mesh,
        in_specs=(P("dp", "mp"), P("dp", "mp"), P("dp", "mp"), P("dp"), P("dp"), P("dp", "mp")),
        out_specs=P("dp", "mp"),
        check_vma=False,
    )
```

```python
import functools
import math

import jax
import jax.numpy as jnp
from jax import lax
from jax.experimental import pallas as pl
from jax.experimental.pallas import tpu as pltpu
from jax.sharding import PartitionSpec as P

HEAD_SIZE = 128
BLOCK = 128
NB = 24
MESH = pl.DeviceIdType.MESH
MASKED = -1e30
VMEM = 60 * 1024 * 1024


def attend_kernel(per_owner, plan_ref, queries_ref, keys_ref, values_ref, ids_ref, out_ref):
    step = pl.program_id(0)
    repeat = queries_ref.shape[1] // HEAD_SIZE
    factor = math.log2(math.e) / math.sqrt(HEAD_SIZE)
    row_at = lax.broadcasted_iota(jnp.int32, (BLOCK, BLOCK), 0)
    col_at = lax.broadcasted_iota(jnp.int32, (BLOCK, BLOCK), 1)
    causal = col_at <= row_at
    ones = jnp.ones((BLOCK, HEAD_SIZE), jnp.bfloat16)
    for layer in range(per_owner):
        block = plan_ref[0, step * per_owner + layer]
        rows = pl.ds(pl.multiple_of(block * BLOCK, BLOCK), BLOCK)
        along = jnp.broadcast_to(ids_ref[pl.ds(block, 1), :], (BLOCK, BLOCK))
        down = along.T
        bias = jnp.where((along == down) & causal, 0.0, MASKED)
        value = jnp.where(down >= 0, values_ref[rows, :].astype(jnp.float32), 0.0)
        value = jnp.concatenate([value.astype(jnp.bfloat16), ones], axis=1)
        key = keys_ref[rows, :]
        query = queries_ref[rows, :]
        query = jnp.concatenate(
            [query[:, h * HEAD_SIZE:(h + 1) * HEAD_SIZE] for h in range(repeat)], axis=0
        )
        scores = lax.dot_general(
            query, key, (((1,), (1,)), ((), ())), preferred_element_type=jnp.float32
        )
        weights = []
        for head in range(repeat):
            part = scores[head * BLOCK:(head + 1) * BLOCK] + bias
            highest = jnp.max(part, axis=1, keepdims=True)
            weights.append(jnp.exp2((part - highest) * factor).astype(jnp.bfloat16))
        summed = jnp.dot(
            jnp.concatenate(weights, axis=0), value, preferred_element_type=jnp.float32
        )
        summed = summed[:, :HEAD_SIZE] / summed[:, HEAD_SIZE:]
        for head in range(repeat):
            columns = slice(head * HEAD_SIZE, (head + 1) * HEAD_SIZE)
            out_ref[0, layer, :, columns] = summed[head * BLOCK:(head + 1) * BLOCK].astype(
                out_ref.dtype
            )


def attend(plan, queries, keys, values, ids, members, per_owner):
    cols = queries.shape[1]

    def whole(array):
        return pl.BlockSpec(array.shape, lambda i, c: (0, 0))

    return pl.pallas_call(
        functools.partial(attend_kernel, per_owner),
        out_shape=jax.ShapeDtypeStruct((members, per_owner, BLOCK, cols), jnp.bfloat16),
        grid_spec=pltpu.PrefetchScalarGridSpec(
            num_scalar_prefetch=1,
            grid=(members,),
            in_specs=[whole(queries), whole(keys), whole(values), whole(ids)],
            out_specs=pl.BlockSpec((1, per_owner, BLOCK, cols), lambda i, c: (i, 0, 0, 0)),
        ),
        compiler_params=pltpu.CompilerParams(vmem_limit_bytes=VMEM),
        cost_estimate=pl.CostEstimate(
            flops=members * per_owner * cols * BLOCK * BLOCK * 4,
            bytes_accessed=4 * queries.size,
            transcendentals=members * per_owner * cols * BLOCK,
        ),
    )(plan, queries, keys, values, ids)


def flip(index, mask):
    bit = 1
    while bit <= mask:
        if mask & bit:
            index = index + bit - 2 * bit * ((index // bit) % 2)
        bit *= 2
    return index


def plan_kernel(members, per_owner, count_ref, plan_ref, table_ref, send_sem, recv_sem):
    me = lax.axis_index("dp")
    mine = lax.axis_index("mp")
    barrier = pltpu.get_barrier_semaphore()
    for mask in range(1, members):
        pl.semaphore_signal(
            barrier, inc=1, device_id=(flip(me, mask), mine), device_id_type=MESH
        )
    pl.semaphore_wait(barrier, members - 1)
    copies = [
        pltpu.make_async_remote_copy(
            src_ref=count_ref,
            dst_ref=table_ref.at[me],
            send_sem=send_sem.at[mask],
            recv_sem=recv_sem.at[mask],
            device_id=(flip(me, mask), mine),
            device_id_type=MESH,
        )
        for mask in range(1, members)
    ]
    for copy in copies:
        copy.start()
    own_count = count_ref[...]
    table_ref[me] = own_count
    for copy in copies:
        copy.wait()
    row = lax.broadcasted_iota(jnp.int32, own_count.shape, 0)
    lane = lax.broadcasted_iota(jnp.int32, own_count.shape, 1)
    shift = members.bit_length() - 1
    start = jnp.zeros_like(own_count)
    first = jnp.zeros_like(own_count)
    slots = jnp.zeros_like(own_count)
    wanted = me + lane * members
    for member in range(members):
        count = table_ref[member]
        first = jnp.where(me == member, start, first)
        within = wanted - start
        holds = (within >= 0) & (within < count)
        slots = jnp.where(
            holds, member * per_owner + lax.shift_right_logical(within, shift), slots
        )
        start = start + count
    owner = jnp.zeros_like(lane)
    for member in range(1, members):
        owner = owner + (lane >= member * per_owner).astype(jnp.int32)
    layer = lane - owner * per_owner
    turned = (owner - first + members * NB) & (members - 1)
    chosen = jnp.minimum(turned + layer * members, NB - 1)
    chosen = jnp.maximum(chosen, 0)
    plan_ref[...] = jnp.where(row == 0, chosen, slots)


def make_plan(live_counts, members, per_owner):
    count = jnp.broadcast_to(live_counts[:, None], (8, 128))
    dma = pltpu.SemaphoreType.DMA
    return pl.pallas_call(
        functools.partial(plan_kernel, members, per_owner),
        out_shape=jax.ShapeDtypeStruct(count.shape, jnp.int32),
        in_specs=[pl.BlockSpec(memory_space=pltpu.VMEM)],
        out_specs=pl.BlockSpec(memory_space=pltpu.VMEM),
        scratch_shapes=[
            pltpu.VMEM((members,) + count.shape, jnp.int32), dma((members,)), dma((members,))
        ],
        compiler_params=pltpu.CompilerParams(collective_id=1, has_side_effects=True),
    )(count)


def exchange_kernel(
    members, columns, per_owner,
    sent_ref, weight_ref, far_weight_ref, held_ref, full_ref,
    local_sem, send_dp, recv_dp, send_x, recv_x, send_w, recv_w,
):
    me = lax.axis_index("dp")
    mine = lax.axis_index("mp")
    top = members // 2

    def dp_device(mask):
        return (flip(me, mask), mine)

    def mp_device(mask):
        return (me, flip(mine, mask))

    bits = [1 << b for b in reversed(range(columns.bit_length() - 1))]
    barrier = pltpu.get_barrier_semaphore()
    for mask in range(1, members):
        pl.semaphore_signal(barrier, inc=1, device_id=dp_device(mask), device_id_type=MESH)
    for mask in bits:
        pl.semaphore_signal(barrier, inc=1, device_id=mp_device(mask), device_id_type=MESH)
    pl.semaphore_wait(barrier, members - 1 + len(bits))

    def dp_copy(mask, layer, source):
        return pltpu.make_async_remote_copy(
            src_ref=sent_ref.at[flip(me, mask), layer],
            dst_ref=held_ref.at[mine, source, layer],
            send_sem=send_dp.at[mask, layer],
            recv_sem=recv_dp.at[mask, layer],
            device_id=dp_device(mask),
            device_id_type=MESH,
        )

    def mp_copy(place, bit, mask, layer):
        source = flip(me, mask)
        column = flip(mine, place)
        if mask == 0 and place == 0:
            src = sent_ref.at[source, layer]
        else:
            src = held_ref.at[column, source, layer]
        return pltpu.make_async_remote_copy(
            src_ref=src,
            dst_ref=held_ref.at[column, source, layer],
            send_sem=send_x.at[place ^ bit, mask, layer],
            recv_sem=recv_x.at[place ^ bit, mask, layer],
            device_id=mp_device(bit),
            device_id_type=MESH,
        )

    def weight_copy(mask, bit):
        owner = flip(me, mask)
        if mask == 0:
            src = weight_ref
        elif mask == top:
            src = far_weight_ref
        else:
            src = full_ref.at[owner]
        return pltpu.make_async_remote_copy(
            src_ref=src,
            dst_ref=full_ref.at[owner],
            send_sem=send_w.at[mask ^ bit],
            recv_sem=recv_w.at[mask ^ bit],
            device_id=dp_device(bit),
            device_id_type=MESH,
        )

    local = [
        pltpu.make_async_copy(weight_ref, full_ref.at[me], local_sem.at[0]),
        pltpu.make_async_copy(far_weight_ref, full_ref.at[flip(me, top)], local_sem.at[1]),
        pltpu.make_async_copy(sent_ref.at[me], held_ref.at[mine, me], local_sem.at[2]),
    ]
    started = []

    def start(copy):
        copy.start()
        started.append(copy)

    def spread_weight(mask, below):
        bit = below // 2
        while bit >= 1:
            start(weight_copy(mask, bit))
            bit //= 2

    def spread(place, below, mask, layer):
        for bit in bits:
            if bit < below:
                start(mp_copy(place, bit, mask, layer))

    order = sorted(range(1, members), key=lambda t: (-(bin(t).count("1") % 2), t))
    spread_weight(0, top)
    spread_weight(top, top)
    for layer in range(per_owner):
        spread(0, columns, 0, layer)
        for mask in order:
            start(dp_copy(mask, layer, me))
    for copy in local:
        copy.start()

    chunks = [(0, layer) for layer in range(per_owner)]
    chunks += [(mask, layer) for layer in range(per_owner) for mask in order]
    weights = [t for t in range(1, members) if t != top]
    weights.sort(key=lambda t: (-(t & -t), t))
    lag = 3

    def relay(mask, layer):
        for place in range(1, columns):
            lowest = place & -place
            mp_copy(place ^ lowest, lowest, mask, layer).wait_recv()
            spread(place, lowest, mask, layer)

    for at in range(len(chunks) + lag):
        if at < len(chunks):
            mask, layer = chunks[at]
            if mask:
                dp_copy(mask, layer, me).wait_recv()
                spread(0, columns, mask, layer)
        if at % 3 == 2 and weights:
            arrived = weights.pop(0)
            lowest = arrived & -arrived
            weight_copy(arrived ^ lowest, lowest).wait_recv()
            spread_weight(arrived, lowest)
        if at >= lag:
            relay(*chunks[at - lag])
    for arrived in weights:
        lowest = arrived & -arrived
        weight_copy(arrived ^ lowest, lowest).wait_recv()
        spread_weight(arrived, lowest)
    for copy in started:
        copy.wait_send()
    for copy in local:
        copy.wait()


def exchange(sent, weight, far_weight, members, columns):
    per_owner = sent.shape[1]
    anywhere = pl.BlockSpec(memory_space=pl.ANY)
    dma = pltpu.SemaphoreType.DMA
    return pl.pallas_call(
        functools.partial(exchange_kernel, members, columns, per_owner),
        out_shape=(
            jax.ShapeDtypeStruct((columns,) + sent.shape, sent.dtype),
            jax.ShapeDtypeStruct((members,) + weight.shape, weight.dtype),
        ),
        in_specs=[anywhere] * 3,
        out_specs=(anywhere, anywhere),
        scratch_shapes=[
            dma((3,)),
            dma((members, per_owner)),
            dma((members, per_owner)),
            dma((columns, members, per_owner)),
            dma((columns, members, per_owner)),
            dma((members,)),
            dma((members,)),
        ],
        compiler_params=pltpu.CompilerParams(collective_id=0, has_side_effects=True, vmem_limit_bytes=VMEM),
        cost_estimate=pl.CostEstimate(
            flops=0, bytes_accessed=60 * sent.size, transcendentals=0
        ),
    )(sent, weight, far_weight)


def project_kernel(columns, slots_ref, first_ref, second_ref, weight_ref, out_ref):
    total = None
    for column in range(columns):
        rows = jnp.concatenate([first_ref[column, 0], second_ref[column, 0]], axis=0)
        depth = rows.shape[1]
        part = jnp.dot(
            rows, weight_ref[column * depth:(column + 1) * depth, :],
            preferred_element_type=jnp.float32,
        )
        total = part if total is None else total + part
    out_ref[...] = total.astype(out_ref.dtype)


def project(slots, held, weight, kept):
    columns, total, _, depth = held.shape
    width = weight.shape[1]

    def picked(which):
        return pl.BlockSpec(
            (columns, 1, BLOCK, depth), lambda i, s: (0, s[1, 2 * i + which], 0, 0)
        )

    return pl.pallas_call(
        functools.partial(project_kernel, columns),
        out_shape=jax.ShapeDtypeStruct((kept * BLOCK, width), jnp.bfloat16),
        grid_spec=pltpu.PrefetchScalarGridSpec(
            num_scalar_prefetch=1,
            grid=(kept // 2,),
            in_specs=[
                picked(0),
                picked(1),
                pl.BlockSpec(weight.shape, lambda i, s: (0, 0)),
            ],
            out_specs=pl.BlockSpec((2 * BLOCK, width), lambda i, s: (i, 0)),
        ),
        compiler_params=pltpu.CompilerParams(vmem_limit_bytes=VMEM),
    )(slots, held, held, weight)


def body(members, columns, queries, keys, values, doc_ids, live_counts, out_weight):
    per_owner = (NB + members - 1) // members
    kept = NB * 11 // 12
    half = members // 2
    plan = make_plan(live_counts, members, per_owner)
    plan, near_weight = lax.optimization_barrier((plan, out_weight))
    far_weight = lax.ppermute(
        near_weight, "dp", [(i, (i + half) % members) for i in range(members)]
    )
    sent = attend(
        plan, queries, keys, values, doc_ids.reshape(NB, BLOCK), members, per_owner
    )
    held, full = exchange(sent, out_weight, far_weight, members, columns)
    held = held.reshape(columns, members * per_owner, BLOCK, queries.shape[1])
    full = full.reshape(members * out_weight.shape[0], out_weight.shape[1])
    return project(plan, held, full, kept)


def solution(mesh):
    return jax.shard_map(
        functools.partial(body, mesh.shape["dp"], mesh.shape["mp"]),
        mesh=mesh,
        in_specs=(P("dp", "mp"), P("dp", "mp"), P("dp", "mp"), P("dp"), P("dp"), P("dp", "mp")),
        out_specs=P("dp", "mp"),
        check_vma=False,
    )
```

```python
import functools
import math

import jax
import jax.numpy as jnp
from jax import lax
from jax.experimental import pallas as pl
from jax.experimental.pallas import tpu as pltpu
from jax.sharding import PartitionSpec as P

HEAD_SIZE = 128
BLOCK = 128
NB = 24
MESH = pl.DeviceIdType.MESH
MASKED = -1e30
VMEM = 60 * 1024 * 1024


def attend_kernel(per_owner, plan_ref, queries_ref, keys_ref, values_ref, ids_ref, out_ref):
    step = pl.program_id(0)
    repeat = queries_ref.shape[1] // HEAD_SIZE
    factor = math.log2(math.e) / math.sqrt(HEAD_SIZE)
    row_at = lax.broadcasted_iota(jnp.int32, (BLOCK, BLOCK), 0)
    col_at = lax.broadcasted_iota(jnp.int32, (BLOCK, BLOCK), 1)
    causal = col_at <= row_at
    ones = jnp.ones((BLOCK, HEAD_SIZE), jnp.bfloat16)
    for layer in range(per_owner):
        block = plan_ref[0, step * per_owner + layer]
        rows = pl.ds(pl.multiple_of(block * BLOCK, BLOCK), BLOCK)
        along = jnp.broadcast_to(ids_ref[pl.ds(block, 1), :], (BLOCK, BLOCK))
        down = along.T
        bias = jnp.where((along == down) & causal, 0.0, MASKED)
        value = jnp.where(down >= 0, values_ref[rows, :].astype(jnp.float32), 0.0)
        value = jnp.concatenate([value.astype(jnp.bfloat16), ones], axis=1)
        key = keys_ref[rows, :]
        query = queries_ref[rows, :]
        query = jnp.concatenate(
            [query[:, h * HEAD_SIZE:(h + 1) * HEAD_SIZE] for h in range(repeat)], axis=0
        )
        scores = lax.dot_general(
            query, key, (((1,), (1,)), ((), ())), preferred_element_type=jnp.float32
        )
        weights = []
        for head in range(repeat):
            part = scores[head * BLOCK:(head + 1) * BLOCK] + bias
            highest = jnp.max(part, axis=1, keepdims=True)
            weights.append(jnp.exp2((part - highest) * factor).astype(jnp.bfloat16))
        summed = jnp.dot(
            jnp.concatenate(weights, axis=0), value, preferred_element_type=jnp.float32
        )
        summed = summed[:, :HEAD_SIZE] / summed[:, HEAD_SIZE:]
        for head in range(repeat):
            columns = slice(head * HEAD_SIZE, (head + 1) * HEAD_SIZE)
            out_ref[0, layer, :, columns] = summed[head * BLOCK:(head + 1) * BLOCK].astype(
                out_ref.dtype
            )


def attend(plan, queries, keys, values, ids, members, per_owner):
    cols = queries.shape[1]

    def whole(array):
        return pl.BlockSpec(array.shape, lambda i, c: (0, 0))

    return pl.pallas_call(
        functools.partial(attend_kernel, per_owner),
        out_shape=jax.ShapeDtypeStruct((members, per_owner, BLOCK, cols), jnp.bfloat16),
        grid_spec=pltpu.PrefetchScalarGridSpec(
            num_scalar_prefetch=1,
            grid=(members,),
            in_specs=[whole(queries), whole(keys), whole(values), whole(ids)],
            out_specs=pl.BlockSpec((1, per_owner, BLOCK, cols), lambda i, c: (i, 0, 0, 0)),
        ),
        compiler_params=pltpu.CompilerParams(vmem_limit_bytes=VMEM),
        cost_estimate=pl.CostEstimate(
            flops=members * per_owner * cols * BLOCK * BLOCK * 4,
            bytes_accessed=4 * queries.size,
            transcendentals=members * per_owner * cols * BLOCK,
        ),
    )(plan, queries, keys, values, ids)


def flip(index, mask):
    bit = 1
    while bit <= mask:
        if mask & bit:
            index = index + bit - 2 * bit * ((index // bit) % 2)
        bit *= 2
    return index


def plan_kernel(members, per_owner, count_ref, plan_ref, table_ref, send_sem, recv_sem):
    me = lax.axis_index("dp")
    mine = lax.axis_index("mp")
    barrier = pltpu.get_barrier_semaphore()
    for mask in range(1, members):
        pl.semaphore_signal(
            barrier, inc=1, device_id=(flip(me, mask), mine), device_id_type=MESH
        )
    pl.semaphore_wait(barrier, members - 1)
    copies = [
        pltpu.make_async_remote_copy(
            src_ref=count_ref,
            dst_ref=table_ref.at[me],
            send_sem=send_sem.at[mask],
            recv_sem=recv_sem.at[mask],
            device_id=(flip(me, mask), mine),
            device_id_type=MESH,
        )
        for mask in range(1, members)
    ]
    for copy in copies:
        copy.start()
    own_count = count_ref[...]
    table_ref[me] = own_count
    for copy in copies:
        copy.wait()
    row = lax.broadcasted_iota(jnp.int32, own_count.shape, 0)
    lane = lax.broadcasted_iota(jnp.int32, own_count.shape, 1)
    shift = members.bit_length() - 1
    start = jnp.zeros_like(own_count)
    first = jnp.zeros_like(own_count)
    slots = jnp.zeros_like(own_count)
    wanted = me + lane * members
    for member in range(members):
        count = table_ref[member]
        first = jnp.where(me == member, start, first)
        within = wanted - start
        holds = (within >= 0) & (within < count)
        slots = jnp.where(
            holds, member * per_owner + lax.shift_right_logical(within, shift), slots
        )
        start = start + count
    owner = jnp.zeros_like(lane)
    for member in range(1, members):
        owner = owner + (lane >= member * per_owner).astype(jnp.int32)
    layer = lane - owner * per_owner
    turned = (owner - first + members * NB) & (members - 1)
    chosen = jnp.minimum(turned + layer * members, NB - 1)
    chosen = jnp.maximum(chosen, 0)
    plan_ref[...] = jnp.where(row == 0, chosen, slots)


def make_plan(live_counts, members, per_owner):
    count = jnp.broadcast_to(live_counts[:, None], (8, 128))
    dma = pltpu.SemaphoreType.DMA
    return pl.pallas_call(
        functools.partial(plan_kernel, members, per_owner),
        out_shape=jax.ShapeDtypeStruct(count.shape, jnp.int32),
        in_specs=[pl.BlockSpec(memory_space=pltpu.VMEM)],
        out_specs=pl.BlockSpec(memory_space=pltpu.VMEM),
        scratch_shapes=[
            pltpu.VMEM((members,) + count.shape, jnp.int32), dma((members,)), dma((members,))
        ],
        compiler_params=pltpu.CompilerParams(collective_id=1, has_side_effects=True),
    )(count)


def exchange_kernel(
    members, columns, per_owner,
    sent_ref, weight_ref, far_weight_ref, held_ref, full_ref,
    local_sem, send_dp, recv_dp, send_x, recv_x, send_w, recv_w,
):
    me = lax.axis_index("dp")
    mine = lax.axis_index("mp")
    top = members // 2

    def dp_device(mask):
        return (flip(me, mask), mine)

    def mp_device(mask):
        return (me, flip(mine, mask))

    bits = [1 << b for b in reversed(range(columns.bit_length() - 1))]
    barrier = pltpu.get_barrier_semaphore()
    for mask in range(1, members):
        pl.semaphore_signal(barrier, inc=1, device_id=dp_device(mask), device_id_type=MESH)
    for mask in bits:
        pl.semaphore_signal(barrier, inc=1, device_id=mp_device(mask), device_id_type=MESH)
    pl.semaphore_wait(barrier, members - 1 + len(bits))

    def dp_copy(mask, layer, source):
        return pltpu.make_async_remote_copy(
            src_ref=sent_ref.at[flip(me, mask), layer],
            dst_ref=held_ref.at[mine, source, layer],
            send_sem=send_dp.at[mask, layer],
            recv_sem=recv_dp.at[mask, layer],
            device_id=dp_device(mask),
            device_id_type=MESH,
        )

    def mp_copy(place, bit, mask, layer):
        source = flip(me, mask)
        column = flip(mine, place)
        if mask == 0 and place == 0:
            src = sent_ref.at[source, layer]
        else:
            src = held_ref.at[column, source, layer]
        return pltpu.make_async_remote_copy(
            src_ref=src,
            dst_ref=held_ref.at[column, source, layer],
            send_sem=send_x.at[place ^ bit, mask, layer],
            recv_sem=recv_x.at[place ^ bit, mask, layer],
            device_id=mp_device(bit),
            device_id_type=MESH,
        )

    def weight_copy(mask, bit):
        owner = flip(me, mask)
        if mask == 0:
            src = weight_ref
        elif mask == top:
            src = far_weight_ref
        else:
            src = full_ref.at[owner]
        return pltpu.make_async_remote_copy(
            src_ref=src,
            dst_ref=full_ref.at[owner],
            send_sem=send_w.at[mask ^ bit],
            recv_sem=recv_w.at[mask ^ bit],
            device_id=dp_device(bit),
            device_id_type=MESH,
        )

    local = [
        pltpu.make_async_copy(weight_ref, full_ref.at[me], local_sem.at[0]),
        pltpu.make_async_copy(far_weight_ref, full_ref.at[flip(me, top)], local_sem.at[1]),
        pltpu.make_async_copy(sent_ref.at[me], held_ref.at[mine, me], local_sem.at[2]),
    ]
    started = []

    def start(copy):
        copy.start()
        started.append(copy)

    def spread_weight(mask, below):
        bit = below // 2
        while bit >= 1:
            start(weight_copy(mask, bit))
            bit //= 2

    def spread(place, below, mask, layer):
        for bit in bits:
            if bit < below:
                start(mp_copy(place, bit, mask, layer))

    order = sorted(range(1, members), key=lambda t: (-(bin(t).count("1") % 2), t))
    for layer in range(per_owner):
        spread(0, columns, 0, layer)
        for mask in order:
            start(dp_copy(mask, layer, me))
        if layer == 0:
            spread_weight(0, top)
            spread_weight(top, top)
    for copy in local:
        copy.start()

    chunks = [(0, layer) for layer in range(per_owner)]
    chunks += [(mask, layer) for layer in range(per_owner) for mask in order]
    weights = [t for t in range(1, members) if t != top]
    weights.sort(key=lambda t: (-(t & -t), t))
    lag = 3

    def relay(mask, layer):
        for place in range(1, columns):
            lowest = place & -place
            mp_copy(place ^ lowest, lowest, mask, layer).wait_recv()
            spread(place, lowest, mask, layer)

    for at in range(len(chunks) + lag):
        if at < len(chunks):
            mask, layer = chunks[at]
            if mask:
                dp_copy(mask, layer, me).wait_recv()
                spread(0, columns, mask, layer)
        if at >= members and at % 2 and weights:
            arrived = weights.pop(0)
            lowest = arrived & -arrived
            weight_copy(arrived ^ lowest, lowest).wait_recv()
            spread_weight(arrived, lowest)
        if at >= lag:
            relay(*chunks[at - lag])
    for arrived in weights:
        lowest = arrived & -arrived
        weight_copy(arrived ^ lowest, lowest).wait_recv()
        spread_weight(arrived, lowest)
    for copy in started:
        copy.wait_send()
    for copy in local:
        copy.wait()


def exchange(sent, weight, far_weight, members, columns):
    per_owner = sent.shape[1]
    anywhere = pl.BlockSpec(memory_space=pl.ANY)
    dma = pltpu.SemaphoreType.DMA
    return pl.pallas_call(
        functools.partial(exchange_kernel, members, columns, per_owner),
        out_shape=(
            jax.ShapeDtypeStruct((columns,) + sent.shape, sent.dtype),
            jax.ShapeDtypeStruct((members,) + weight.shape, weight.dtype),
        ),
        in_specs=[anywhere] * 3,
        out_specs=(anywhere, anywhere),
        scratch_shapes=[
            dma((3,)),
            dma((members, per_owner)),
            dma((members, per_owner)),
            dma((columns, members, per_owner)),
            dma((columns, members, per_owner)),
            dma((members,)),
            dma((members,)),
        ],
        compiler_params=pltpu.CompilerParams(collective_id=0, has_side_effects=True, vmem_limit_bytes=VMEM),
        cost_estimate=pl.CostEstimate(
            flops=0, bytes_accessed=60 * sent.size, transcendentals=0
        ),
    )(sent, weight, far_weight)


def project_kernel(columns, slots_ref, first_ref, second_ref, weight_ref, out_ref):
    total = None
    for column in range(columns):
        rows = jnp.concatenate([first_ref[column, 0], second_ref[column, 0]], axis=0)
        depth = rows.shape[1]
        part = jnp.dot(
            rows, weight_ref[column * depth:(column + 1) * depth, :],
            preferred_element_type=jnp.float32,
        )
        total = part if total is None else total + part
    out_ref[...] = total.astype(out_ref.dtype)


def project(slots, held, weight, kept):
    columns, total, _, depth = held.shape
    width = weight.shape[1]

    def picked(which):
        return pl.BlockSpec(
            (columns, 1, BLOCK, depth), lambda i, s: (0, s[1, 2 * i + which], 0, 0)
        )

    return pl.pallas_call(
        functools.partial(project_kernel, columns),
        out_shape=jax.ShapeDtypeStruct((kept * BLOCK, width), jnp.bfloat16),
        grid_spec=pltpu.PrefetchScalarGridSpec(
            num_scalar_prefetch=1,
            grid=(kept // 2,),
            in_specs=[
                picked(0),
                picked(1),
                pl.BlockSpec(weight.shape, lambda i, s: (0, 0)),
            ],
            out_specs=pl.BlockSpec((2 * BLOCK, width), lambda i, s: (i, 0)),
        ),
        compiler_params=pltpu.CompilerParams(vmem_limit_bytes=VMEM),
    )(slots, held, held, weight)


def body(members, columns, queries, keys, values, doc_ids, live_counts, out_weight):
    per_owner = (NB + members - 1) // members
    kept = NB * 11 // 12
    half = members // 2
    plan = make_plan(live_counts, members, per_owner)
    plan, near_weight = lax.optimization_barrier((plan, out_weight))
    far_weight = lax.ppermute(
        near_weight, "dp", [(i, (i + half) % members) for i in range(members)]
    )
    sent = attend(
        plan, queries, keys, values, doc_ids.reshape(NB, BLOCK), members, per_owner
    )
    held, full = exchange(sent, out_weight, far_weight, members, columns)
    held = held.reshape(columns, members * per_owner, BLOCK, queries.shape[1])
    full = full.reshape(members * out_weight.shape[0], out_weight.shape[1])
    return project(plan, held, full, kept)


def solution(mesh):
    return jax.shard_map(
        functools.partial(body, mesh.shape["dp"], mesh.shape["mp"]),
        mesh=mesh,
        in_specs=(P("dp", "mp"), P("dp", "mp"), P("dp", "mp"), P("dp"), P("dp"), P("dp", "mp")),
        out_specs=P("dp", "mp"),
        check_vma=False,
    )
```
